32 devices in a mesh: ctx: 8 (over z, x), dp: 4 (over y, core).
Axes of the slice: x: 2, y: 2, z: 4, core: 2. Of those that a mesh axis runs over, the one named last changes fastest.
Arguments:
- head_input: bfloat16 [8192, 4096], P(('dp', 'ctx')), parts along dimension 0, may hold values from -6 to 6
- gate_input: bfloat16 [8192, 4096], P(('dp', 'ctx')), parts along dimension 0, may hold values from -6 to 6
- write_vector: bfloat16 [8192, 128], P(('dp', 'ctx')), parts along dimension 0, may hold values from -2.5 to 2.5
- read_vector: bfloat16 [8192, 128], P(('dp', 'ctx')), parts along dimension 0, may hold values from -2.5 to 2.5
- increment_preactivation: bfloat16 [8192, 64], P(('dp', 'ctx')), parts along dimension 0, may hold values from -2 to 8
- step_bias: float32 [64], replicated, may hold values from -1 to 0.5
- decay_log: float32 [64], replicated, may hold values from -9.3 to -2.3
- skip_gain: float32 [64], replicated, may hold values from 0.5 to 1.5
- norm_weight: float32 [4096], replicated, may hold values from 0.5 to 1.5
- doc_starts: int32 [64], P(('dp', 'ctx')), parts along dimension 0, may hold values from 0 to 1, as said below
- block_order: int32 [64], P(('dp', 'ctx')), parts along dimension 0, may hold values from 0 to 15, as said below
Outputs:
- packed_out: bfloat16 [8192, 4096], P(('dp', 'ctx')), parts along dimension 0
The draws below stay inside these ranges and needn't reach their ends.
There are 4 independent parts, one for each index of `dp`. The reference program is written for one: setup_inputs(seed, part) draws one part's arguments, and reference() takes and returns one part's arrays. A program takes and returns all parts, laid end to end along the dimension named above; an argument that names none is the same for every part. Nothing has to cross between parts.
Inputs may be any that keep to these rules, and one draw needn't show every extreme that they name: `doc_starts`: block 0 starts a document; no document is longer than 128 blocks. `block_order`: a permutation of the block indices that keeps each document's blocks together and in their order.
All inputs are finite; a program needn't handle non-finite values.
Results may differ from the reference program's by a relative error of at most 0.0085.
Values may be sent and summed in bfloat16 or wider, within the bound.
No kernel may reach another device: no remote copies, remote signals or barrier semaphores. Data moves between devices by JAX's collectives and lax.ppermute only.
A program may use at most 128 MiB of HBM per device.

```python
import math
import jax
import jax.numpy as jnp
from jax import lax

HEADS = 64
HEAD_DIM = 64
STATE = 128
GROUP = 128
DOC_MOST = 128
JOINED_TERMS = 2048


def doc_tables(key):
    key_baseline = jax.random.fold_in(key, 7)
    key_start, key_rank, key_extra = jax.random.split(key_baseline, 3)
    block_count = JOINED_TERMS // GROUP
    positions = jnp.arange(block_count, dtype=jnp.int32)
    chosen = jax.random.randint(key_start, (block_count,), 0, 64) == 0
    extra_at = jax.random.randint(key_extra, (4,), 1, block_count)
    hit_extra = jnp.any(positions[:, None] == extra_at[None, :], axis=1)
    forced = jnp.logical_or(positions % DOC_MOST == 0, hit_extra)
    starts = jnp.logical_or(chosen, forced).astype(jnp.int32)
    segment_number = jnp.cumsum(starts) - 1
    ranks = jax.random.randint(key_rank, (block_count,), 0, 1 << 20)
    priority = ranks[segment_number] * block_count + positions
    permuted = jnp.argsort(priority, stable=True).astype(jnp.int32)
    return (starts, permuted)


def draw_doc_starts(key, part):
    return doc_tables(key)[0]


def draw_block_order(key, part):
    return doc_tables(key)[1]


def draw_increment_preactivation(key, part):
    key_baseline = jax.random.fold_in(key, 11)
    key_value_product, lookup_jump = jax.random.split(key_baseline)
    spike_series = (jax.random.randint(lookup_jump, (JOINED_TERMS, 1), 0, 64) == 0).astype(jnp.float32)
    payload_reference_level = jnp.clip(0.5 * jax.random.normal(key_value_product, (JOINED_TERMS, HEADS), jnp.float32), -2.0, 2.0)
    return (payload_reference_level + 6.0 * spike_series).astype(jnp.bfloat16)


def draw_decay_log(key, part):
    key_baseline = jax.random.fold_in(key, 13)
    return jax.random.uniform(key_baseline, (HEADS,), jnp.float32, math.log(0.0003), math.log(0.1))


def levels(own_key, dims, shards, low, largest):
    gain = 1.0
    for axis_at, blocks in shards:
        steps = jax.random.uniform(jax.random.fold_in(jax.random.fold_in(own_key, 6), axis_at), (blocks,), jnp.float32, low / len(shards), largest / len(shards))
        gain = gain * jnp.repeat(jnp.exp(steps), dims[axis_at] // blocks).reshape((-1,) + (1,) * (len(dims) - 1 - axis_at))
    return gain


def noise(stream_key, extent, scale, reach, cuts=(), kind=jnp.bfloat16):
    entries = scale * jax.random.normal(stream_key, extent, jnp.float32)
    if cuts:
        entries = entries * levels(stream_key, extent, cuts, -0.22, 0.18)
    return jnp.clip(entries, -reach, reach).astype(kind)


def setup_inputs(seed: int = 0, part: int = 0) -> dict:
    streams_of = jax.random.split(jax.random.key(seed), 12)
    part_keys = jax.random.split(jax.random.fold_in(streams_of[11], part), 12)
    return {
        "head_input": noise(part_keys[0], (JOINED_TERMS, HEADS * HEAD_DIM), 1.0, 6.0, ((0, 8),)),
        "gate_input": noise(part_keys[1], (JOINED_TERMS, HEADS * HEAD_DIM), 1.0, 6.0, ((0, 8),)),
        "write_vector": noise(part_keys[2], (JOINED_TERMS, STATE), 0.3, 2.5, ((0, 8),)),
        "read_vector": noise(part_keys[3], (JOINED_TERMS, STATE), 0.3, 2.5, ((0, 8),)),
        "increment_preactivation": draw_increment_preactivation(jax.random.fold_in(jax.random.fold_in(streams_of[11], part), 71), part),
        "step_bias": jnp.clip(jax.random.uniform(streams_of[5], (HEADS,), jnp.float32, -1.0, 0.5), -1.0, 0.5),
        "decay_log": draw_decay_log(jax.random.fold_in(streams_of[11], 71), part),
        "skip_gain": jnp.clip(jax.random.uniform(streams_of[7], (HEADS,), jnp.float32, 0.5, 1.5), 0.5, 1.5),
        "norm_weight": jnp.clip(1.0 + 0.1 * jax.random.normal(streams_of[8], (HEADS * HEAD_DIM,), jnp.float32), 0.5, 1.5),
        "doc_starts": draw_doc_starts(jax.random.fold_in(jax.random.fold_in(streams_of[11], part), 71), part),
        "block_order": draw_block_order(jax.random.fold_in(jax.random.fold_in(streams_of[11], part), 71), part),
    }


highest = lax.Precision.HIGHEST

def product(form, left, right):
    return jnp.einsum(form, left.astype(jnp.float32), right.astype(jnp.float32), precision=highest)

def link_maps(earlier, current):
    decay_one, state_one = earlier
    decay_two, state_two = current
    return (decay_one * decay_two, decay_two[..., None, None] * state_one + state_two)

def group_terms(inputs, step_size, decay_speed, scores, write_vector, keep_mask, group_size):
    length, local_heads, head_width = inputs.shape
    group_count = length // group_size
    blocked = inputs.reshape(group_count, group_size, local_heads, head_width)
    steps_blocked = step_size.reshape(group_count, group_size, local_heads).transpose(0, 2, 1)
    cumulative = jnp.cumsum(-steps_blocked * decay_speed[None, :, None], axis=2)
    row_labels = lax.broadcasted_iota(jnp.int32, (group_size, group_size), 0)
    col_ids = lax.broadcasted_iota(jnp.int32, (group_size, group_size), 1)
    gap_log = cumulative[:, :, :, None] - cumulative[:, :, None, :]
    decays = jnp.exp(jnp.where(row_labels >= col_ids, gap_log, -jnp.inf))
    weight = (scores[:, None, :, :] * decays * steps_blocked[:, :, None, :]).astype(jnp.bfloat16)
    local_out = product('chij,cjhp->cihp', weight, blocked)
    last_cum = cumulative[:, :, -1]
    tail_decay = jnp.exp(last_cum[:, :, None] - cumulative) * steps_blocked
    scaled = (blocked.astype(jnp.float32) * tail_decay.transpose(0, 2, 1)[..., None]).astype(jnp.bfloat16)
    write_blocked = write_vector.reshape(group_count, group_size, -1)
    states = product('cjhp,cjn->chpn', scaled, write_blocked)
    factor = jnp.exp(last_cum) * keep_mask[:, None]
    scan_decay, scan_state = lax.associative_scan(link_maps, (factor, states))
    return (local_out, cumulative, scan_decay, scan_state)

def finish_groups(local_out, cumulative, scan_decay, scan_state, keep_mask, read_vector, starting_entry, inputs, skip_gain):
    group_count, group_size, local_heads, head_width = local_out.shape
    prior_decay = jnp.concatenate([jnp.ones((1, local_heads), jnp.float32), scan_decay[:-1]], 0)
    prior_state = jnp.concatenate([jnp.zeros((1,) + scan_state.shape[1:], jnp.float32), scan_state[:-1]], 0)
    entering = keep_mask[:, None, None, None] * (prior_decay[:, :, None, None] * starting_entry[None] + prior_state)
    read_blocked = read_vector.reshape(group_count, group_size, -1)
    carried = product('cin,chpn->cihp', read_blocked, entering)
    carried = carried * jnp.exp(cumulative).transpose(0, 2, 1)[..., None]
    blocked = inputs.reshape(local_out.shape).astype(jnp.float32)
    result = local_out + carried + skip_gain[None, None, :, None] * blocked
    return result.reshape(group_count * group_size, local_heads * head_width)

def gated_norm(gated, norm_weight):
    values = gated.astype(jnp.float32)
    mean_square = lax.optimization_barrier(jnp.mean(values * values, axis=-1, keepdims=True))
    return (values * lax.rsqrt(mean_square + 1e-05) * norm_weight).astype(jnp.bfloat16)

def reference(head_input, gate_input, write_vector, read_vector, increment_preactivation, step_bias, decay_log, skip_gain, norm_weight, doc_starts, block_order):
    step_size = jax.nn.softplus(increment_preactivation.astype(jnp.float32) + step_bias)
    decay_speed = jnp.exp(decay_log)
    keep_mask = 1.0 - doc_starts.astype(jnp.float32)
    group_count = JOINED_TERMS // GROUP
    scores = product('cin,cjn->cij', read_vector.reshape(group_count, GROUP, -1), write_vector.reshape(group_count, GROUP, -1))
    per_head = head_input.reshape(JOINED_TERMS, HEADS, HEAD_DIM).transpose(1, 0, 2)[:, :, None, :]

    def one_head(pieces):
        inputs, head_steps, attention_forgetting, head_gain = pieces
        local_out, cumulative, scan_decay, scan_state = group_terms(inputs, head_steps[:, None], attention_forgetting[None], scores, write_vector, keep_mask, GROUP)
        starting_entry = jnp.zeros((1, HEAD_DIM, STATE), jnp.float32)
        return finish_groups(local_out, cumulative, scan_decay, scan_state, keep_mask, read_vector, starting_entry, inputs, head_gain[None])
    outputs = lax.map(one_head, (per_head, step_size.T, decay_speed, skip_gain))
    combined = outputs.transpose(1, 0, 2).reshape(JOINED_TERMS, HEADS * HEAD_DIM)
    gated = (combined * jax.nn.silu(gate_input.astype(jnp.float32))).astype(jnp.bfloat16)
    normed = gated_norm(gated, norm_weight)
    return normed.reshape(group_count, GROUP, -1)[block_order].reshape(JOINED_TERMS, HEADS * HEAD_DIM)
```

```python
import functools

import jax
import jax.numpy as jnp
from jax import lax
from jax.experimental import pallas as pl
from jax.experimental.pallas import tpu as pltpu
from jax.sharding import PartitionSpec as P

HEAD_DIM = 64
GROUP = 128
LANES = 128
META_ROWS = 16
CHUNK = 512

f32 = jnp.float32
bf16 = jnp.bfloat16
highest = lax.Precision.HIGHEST


def dot(left, right, left_dim=1, right_dim=0, precision=None):
    return lax.dot_general(
        left,
        right,
        (((left_dim,), (right_dim,)), ((), ())),
        precision=precision,
        preferred_element_type=f32,
    )


def run(body, scalars, grid, ins, in_specs, outs, out_specs, scratch=(), name=None):
    return pl.pallas_call(
        body,
        grid_spec=pltpu.PrefetchScalarGridSpec(
            num_scalar_prefetch=1,
            grid=grid,
            in_specs=in_specs,
            out_specs=out_specs,
            scratch_shapes=list(scratch),
        ),
        out_shape=outs,
        name=name,
        compiler_params=pltpu.CompilerParams(
            dimension_semantics=("arbitrary",) * len(grid),
            vmem_limit_bytes=48 * 1024 * 1024,
        ),
    )(scalars, *ins)


def whole(shape):
    return pl.BlockSpec(shape, lambda *a: (0,) * len(shape))


def pack(scalars, array, width, members, parts, part):
    tokens = array.shape[0]

    def body(sc, *refs):
        half = len(refs) // 2
        for src, dst in zip(refs[:half], refs[half:]):
            dst[...] = src[...]

    specs = [
        pl.BlockSpec((tokens, width), lambda i, sc, s=s: (0, (sc[0] ^ s) * parts + part))
        for s in range(1, members)
    ]
    return run(
        body,
        scalars,
        (1,),
        [array] * (members - 1),
        specs,
        [jax.ShapeDtypeStruct((tokens, width), array.dtype)] * (members - 1),
        [whole((tokens, width))] * (members - 1),
        name="pack",
    )


def pick(step, refs, take):
    for number, ref in enumerate(refs):

        @pl.when(step == number)
        def _(ref=ref):
            take(ref)


def prep(scalars, extras, bias, rate, heads, tokens, state):
    members = len(extras)
    rows = extras[0].shape[0]
    total = members * tokens
    groups = tokens // GROUP

    def body(sc, *refs):
        ex, (bias_ref, rate_ref) = refs[:members], refs[members : members + 2]
        logit_refs = refs[members + 2 : 2 * members + 2]
        proj, dt_t, cum_t, dt_c, cum_c, logit_s = refs[2 * members + 2 :]
        who = pl.program_id(0) ^ sc[0]

        def take(ref):
            proj[...] = ref[:tokens, :]

        pick(who, ex, take)

        def take_logit(ref):
            logit_s[...] = ref[...].astype(f32)

        pick(who, logit_refs, take_logit)
        value = logit_s[...] + bias_ref[...]
        step = jnp.maximum(value, 0.0) + jnp.log1p(jnp.exp(-jnp.abs(value)))
        upper = (
            lax.broadcasted_iota(jnp.int32, (GROUP, GROUP), 0)
            <= lax.broadcasted_iota(jnp.int32, (GROUP, GROUP), 1)
        ).astype(f32)
        fall = -step * rate_ref[...]
        dt_t[...] = step
        for g in range(groups):
            part = slice(g * GROUP, (g + 1) * GROUP)
            cumulative = dot(fall[:, part], upper, precision=highest)
            cum_t[:, part] = cumulative
            cum_c[part, :] = cumulative.T
            dt_c[part, :] = step[:, part].T

    logits = [
        e[tokens : rows - META_ROWS].reshape(heads, tokens) for e in extras
    ]
    return run(
        body,
        scalars,
        (members,),
        [*extras, bias, rate, *logits],
        [whole((rows, 2 * state))] * members
        + [whole((heads, 1))] * 2
        + [whole((heads, tokens))] * members,
        [
            jax.ShapeDtypeStruct((total, 2 * state), bf16),
            jax.ShapeDtypeStruct((heads, total), f32),
            jax.ShapeDtypeStruct((heads, total), f32),
            jax.ShapeDtypeStruct((total, heads), f32),
            jax.ShapeDtypeStruct((total, heads), f32),
        ],
        [
            pl.BlockSpec((tokens, 2 * state), lambda i, sc: (i, 0)),
            pl.BlockSpec((heads, tokens), lambda i, sc: (0, i)),
            pl.BlockSpec((heads, tokens), lambda i, sc: (0, i)),
            pl.BlockSpec((tokens, heads), lambda i, sc: (i, 0)),
            pl.BlockSpec((tokens, heads), lambda i, sc: (i, 0)),
        ],
        [pltpu.VMEM((heads, tokens), f32)],
        name="prep",
    )


def ssd(scalars, prepped, xs, gates, first, gain, width, parts, part, want_out):
    proj, dt_t, cum_t, dt_c, cum_c = prepped
    members = len(xs)
    heads = dt_t.shape[0]
    tokens = xs[1].shape[0] if members > 1 else xs[0].shape[0]
    state = proj.shape[1] // 2
    groups = tokens // GROUP
    pairs = width // LANES
    head_of = LANES // HEAD_DIM
    base = part * (width // HEAD_DIM)

    def body(sc, *refs):
        refs = list(refs)
        x_refs = [refs.pop(0) for _ in range(members)]
        if want_out:
            g_refs = [refs.pop(0) for _ in range(members)]
            first_ref, gain_ref = refs.pop(0), refs.pop(0)
        proj_r, dtt, cumt, dtc, cumc = [refs.pop(0) for _ in range(5)]
        out = refs.pop(0)
        carry, x_s, scaled_s = [refs.pop(0) for _ in range(3)]
        g_s = refs.pop(0) if want_out else None
        src = pl.program_id(0)
        who = src ^ sc[0]

        @pl.when(src == 0)
        def _():
            if want_out:
                carry[...] = first_ref[...].astype(f32)
            else:
                carry[...] = jnp.zeros_like(carry)

        def take_x(ref):
            x_s[...] = ref[...]

        pick(who, x_refs, take_x)
        if want_out:

            def take_g(ref):
                g_s[...] = ref[...]

            pick(who, g_refs, take_g)
            lower = lax.broadcasted_iota(jnp.int32, (GROUP, GROUP), 0) >= (
                lax.broadcasted_iota(jnp.int32, (GROUP, GROUP), 1)
            )
        left = lax.broadcasted_iota(jnp.int32, (GROUP, LANES), 1) < HEAD_DIM

        for g in range(groups):
            rows = slice(g * GROUP, (g + 1) * GROUP)
            write = proj_r[rows, :state]
            keep = 1.0 - sc[1 + who * groups + g].astype(f32)
            if want_out:
                read = proj_r[rows, state:]
                scores = dot(read, write, 1, 1)
                carried = dot(read, (carry[...] * keep).astype(bf16))
            for p in range(pairs):
                lanes = slice(p * LANES, (p + 1) * LANES)
                h = base + head_of * p
                x = x_s[rows, lanes]
                xf = x.astype(f32)
                cols = [cumc[rows, h + k : h + k + 1] for k in range(head_of)]
                cum = jnp.where(left, cols[0], cols[1])
                step = jnp.where(left, dtc[rows, h : h + 1], dtc[rows, h + 1 : h + 2])
                last = cum[GROUP - 1 :, :]
                scaled_s[:, lanes] = (xf * jnp.exp(last - cum) * step).astype(bf16)
                if want_out:
                    weights = []
                    for k in range(head_of):
                        gap = cols[k] - cumt[h + k : h + k + 1, rows]
                        decay = jnp.exp(jnp.where(lower, gap, -jnp.inf))
                        weights.append(
                            (scores * decay * dtt[h + k : h + k + 1, rows]).astype(bf16)
                        )
                    zero = jnp.zeros_like(x)
                    local = dot(
                        jnp.concatenate(weights, 1),
                        jnp.concatenate(
                            [jnp.where(left, x, zero), jnp.where(left, zero, x)], 0
                        ),
                    )
                    mixed = local + jnp.exp(cum) * carried[:, lanes] + gain_ref[:, lanes] * xf
                    gate = g_s[rows, lanes].astype(f32)
                    out[rows, lanes] = (mixed * (gate / (1.0 + jnp.exp(-gate)))).astype(bf16)
                carry[:, lanes] = carry[:, lanes] * (jnp.exp(last) * keep)
            carry[...] += dot(write, scaled_s[...], 0, 0)

        if not want_out:
            out[...] = carry[...].astype(bf16)

    own = pl.BlockSpec((tokens, width), lambda i, sc: (0, sc[0] * parts + part))
    pieces = [own] + [whole((tokens, width))] * (members - 1)
    ins, in_specs = list(xs), list(pieces)
    if want_out:
        ins += [*gates, first, gain]
        in_specs += [*pieces, whole((state, width)), pl.BlockSpec((1, width), lambda i, sc: (0, part))]
    ins += [proj, dt_t, cum_t, dt_c, cum_c]
    in_specs += [
        pl.BlockSpec((tokens, 2 * state), lambda i, sc: (i, 0)),
        pl.BlockSpec((heads, tokens), lambda i, sc: (0, i)),
        pl.BlockSpec((heads, tokens), lambda i, sc: (0, i)),
        pl.BlockSpec((tokens, heads), lambda i, sc: (i, 0)),
        pl.BlockSpec((tokens, heads), lambda i, sc: (i, 0)),
    ]
    scratch = [
        pltpu.VMEM((state, width), f32),
        pltpu.VMEM((tokens, width), bf16),
        pltpu.VMEM((GROUP, width), bf16),
    ]
    if want_out:
        outs = jax.ShapeDtypeStruct((members * tokens, width), bf16)
        out_specs = pl.BlockSpec((tokens, width), lambda i, sc: (i, 0))
        scratch.append(pltpu.VMEM((tokens, width), bf16))
    else:
        outs = jax.ShapeDtypeStruct((state, width), bf16)
        out_specs = whole((state, width))
    return run(
        body, scalars, (members,), ins, in_specs, outs, out_specs, scratch,
        name="mix" if want_out else "end_state",
    )


def select(scalars, order_at, members, per, halves):
    total, width = halves[0].shape
    blocks = total // GROUP

    def body(sc, *refs):
        sources, dests = refs[: len(halves)], refs[len(halves) :]
        for s in range(members):
            for i in range(per):
                block = sc[order_at + s * per + i]
                segment = (block // blocks - sc[order_at - 1]) % len(halves)
                start = pl.multiple_of((block % blocks) * GROUP, GROUP)
                into = slice(i * GROUP, (i + 1) * GROUP)

                def take(ref, s=s, start=start, into=into):
                    dests[s][into, :] = ref[pl.ds(start, GROUP), :]

                pick(segment, sources, take)

    return run(
        body,
        scalars,
        (1,),
        halves,
        [whole((total, width))] * len(halves),
        [jax.ShapeDtypeStruct((per * GROUP, width), bf16)] * members,
        [whole((per * GROUP, width))] * members,
        name="select",
    )


def finish(scalars, pieces, norm_weight, width, parts, tokens, features):
    members = len(pieces[0])
    tile = GROUP // 2
    flat = [piece for row in pieces for piece in row]

    def body(sc, *refs):
        ins, weight, out = refs[:-2], refs[-2], refs[-1]
        total = jnp.zeros((tile, LANES), f32)
        for ref in ins:
            value = ref[...].astype(f32)
            square = value * value
            for at in range(width // LANES):
                total = total + square[:, at * LANES : (at + 1) * LANES]
        scale = lax.rsqrt(jnp.sum(total, 1, keepdims=True) / features + 1e-05)
        for part in range(parts):
            for s in range(members):
                start = pl.multiple_of(((sc[0] ^ s) * parts + part) * width, LANES)
                value = ins[part * members + s][...].astype(f32)
                out[:, pl.ds(start, width)] = (
                    value * scale * weight[:, pl.ds(start, width)]
                ).astype(bf16)

    return run(
        body,
        scalars,
        (tokens // tile,),
        [*flat, norm_weight[None, :]],
        [pl.BlockSpec((tile, width), lambda i, sc: (i, 0))] * len(flat) + [whole((1, features))],
        jax.ShapeDtypeStruct((tokens, features), bf16),
        pl.BlockSpec((tile, features), lambda i, sc: (i, 0)),
        name="finish",
    )


def local(
    head_input,
    gate_input,
    write_vector,
    read_vector,
    increment_preactivation,
    step_bias,
    decay_log,
    skip_gain,
    norm_weight,
    doc_starts,
    block_order,
    *,
    segments,
):
    devices = lax.axis_size("ctx")
    members = devices // segments
    tokens, features = head_input.shape
    state = write_vector.shape[1]
    all_heads = step_bias.shape[0]
    heads = all_heads // members
    columns = features // members
    width = min(CHUNK, columns)
    parts = columns // width
    per = doc_starts.shape[0]
    index = lax.axis_index("ctx")
    segment, me = index // members, index % members

    def shift(value, s):
        pairs = [
            (g * members + i, g * members + (i ^ s))
            for g in range(segments)
            for i in range(members)
        ]
        return lax.ppermute(value, "ctx", pairs)

    logits = increment_preactivation.T.reshape(members, heads, tokens)
    meta = jnp.concatenate([doc_starts, block_order // GROUP, block_order % GROUP])
    meta = jnp.pad(meta.astype(bf16), (0, META_ROWS * 2 * state - 3 * per))
    meta = meta.reshape(META_ROWS, 2 * state)
    both = jnp.concatenate([write_vector, read_vector], 1)
    extras = []
    for s in range(members):
        logit = lax.dynamic_index_in_dim(logits, me ^ s, 0, keepdims=False)
        extra = jnp.concatenate([both, logit.reshape(-1, 2 * state), meta], 0)
        extras.append(shift(extra, s) if s else extra)

    my = me.astype(jnp.int32)[None]
    x_parts = []
    g_parts = []
    for k in range(parts):
        x_sent = pack(my, head_input, width, members, parts, k)
        g_sent = pack(my, gate_input, width, members, parts, k)
        x_parts.append([head_input] + [shift(v, s + 1) for s, v in enumerate(x_sent)])
        g_parts.append([gate_input] + [shift(v, s + 1) for s, v in enumerate(g_sent)])

    tables = jnp.stack([e[-META_ROWS, : 3 * per] for e in extras]).astype(f32).astype(jnp.int32)
    starts = tables[:, :per].reshape(-1)
    order = (tables[:, per : 2 * per] * GROUP + tables[:, 2 * per :]).reshape(-1)
    scalars = jnp.concatenate([my, starts, segment.astype(jnp.int32)[None], order])
    order_at = 2 + starts.shape[0]

    def mine(vector):
        return lax.dynamic_slice_in_dim(vector, me * heads, heads)

    bias, rate = mine(step_bias)[:, None], jnp.exp(mine(decay_log))[:, None]
    gain = jnp.repeat(mine(skip_gain), HEAD_DIM)[None, :]
    prepped = prep(my, extras, bias, rate, heads, tokens, state)

    pieces = []
    for k in range(parts):
        args = (scalars, prepped, x_parts[k])
        first = jnp.zeros((state, width), bf16)
        if segments == 2:
            end = ssd(*args, None, None, None, width, parts, k, False)
            first = lax.ppermute(end, "ctx", [(i, i + members) for i in range(members)])
        out = ssd(*args, g_parts[k], first, gain, width, parts, k, True)
        halves = [out]
        if segments == 2:
            swap = [(i, (i + members) % devices) for i in range(devices)]
            halves.append(lax.ppermute(out, "ctx", swap))
        sent = select(scalars, order_at, members, per, halves)
        pieces.append([sent[0]] + [shift(sent[s], s) for s in range(1, members)])
    return finish(my, pieces, norm_weight, width, parts, tokens, features)


def solution(mesh):
    rows = P(("dp", "ctx"), None)
    segments = 2 if mesh.shape["ctx"] >= 4 else 1
    return jax.shard_map(
        functools.partial(local, segments=segments),
        mesh=mesh,
        in_specs=(rows,) * 5 + (P(),) * 4 + (P(("dp", "ctx")),) * 2,
        out_specs=rows,
        check_vma=False,
    )
```

```python
import jax
import jax.numpy as jnp
from jax import lax
from jax.experimental import pallas as pl
from jax.experimental.pallas import tpu as pltpu
from jax.sharding import PartitionSpec as P


HEAD_DIM = 64
GROUP = 128
LANES = 128
META_ROWS = 16
CHUNKS = (256, 256, 256, 256)
SIDE = 2
MEMBER, SEGMENT, ROW, COL = range(4)
MIB = 1024 * 1024

f32 = jnp.float32
bf16 = jnp.bfloat16
highest = lax.Precision.HIGHEST


def chunks(columns):
    if sum(CHUNKS) != columns:
        width = next(w for w in (256, 128) if columns % w == 0)
        return [(at, width) for at in range(0, columns, width)]
    return [(sum(CHUNKS[:k]), width) for k, width in enumerate(CHUNKS)]


def dot(left, right, left_dim=1, right_dim=0, precision=None):
    return lax.dot_general(
        left,
        right,
        (((left_dim,), (right_dim,)), ((), ())),
        precision=precision,
        preferred_element_type=f32,
    )


def run(body, scalars, grid, ins, in_specs, outs, out_specs, scratch=(), mib=8):
    return pl.pallas_call(
        body,
        grid_spec=pltpu.PrefetchScalarGridSpec(
            num_scalar_prefetch=len(scalars),
            grid=grid,
            in_specs=in_specs,
            out_specs=out_specs,
            scratch_shapes=list(scratch),
        ),
        out_shape=outs,
        compiler_params=pltpu.CompilerParams(
            dimension_semantics=("arbitrary",) * len(grid),
            vmem_limit_bytes=mib * MIB,
        ),
    )(*scalars, *ins)


def whole(shape):
    return pl.BlockSpec(shape, lambda *a: (0,) * len(shape))


def pick(step, refs, take):
    for number, ref in enumerate(refs):

        @pl.when(step == number)
        def _(ref=ref):
            take(ref)


def pack(my, arrays, wanted, members, columns, after=()):
    tokens = arrays[0].shape[0]
    total = members * sum(len(numbers) for numbers, _, _ in wanted)

    def body(my_ref, *refs):
        outs, sem = refs[-members * len(wanted) - 1 : -1], refs[-1]
        copies = []
        for w, (numbers, offset, width) in enumerate(wanted):
            for s in range(members):
                start = pl.multiple_of((my_ref[MEMBER] ^ s) * columns + offset, LANES)
                for a, number in enumerate(numbers):
                    copies.append(
                        pltpu.make_async_copy(
                            refs[number].at[:, pl.ds(start, width)],
                            outs[w * members + s].at[pl.ds(a * tokens, tokens), :],
                            sem.at[len(copies)],
                        )
                    )
        for copy in copies:
            copy.start()
        for copy in copies:
            copy.wait()

    out = run(
        body,
        (my,),
        (1,),
        [*arrays, *after],
        [pl.BlockSpec(memory_space=pl.ANY)] * (len(arrays) + len(after)),
        [
            jax.ShapeDtypeStruct((len(numbers) * tokens, width), arrays[0].dtype)
            for numbers, _, width in wanted
            for _ in range(members)
        ],
        [pl.BlockSpec(memory_space=pl.ANY)] * (members * len(wanted)),
        [pltpu.SemaphoreType.DMA((total,))],
        mib=2,
    )
    return [out[w * members : (w + 1) * members] for w in range(len(wanted))]


def gather_small(my, write_vector, read_vector, logits, doc_starts, block_order):
    tokens, state = write_vector.shape
    heads = logits.shape[0]
    groups = tokens // GROUP
    per = doc_starts.shape[0]
    meta_at = 2 * tokens + groups * heads
    rows = meta_at + META_ROWS

    def body(my_ref, write, read, logit, starts, order, out):
        out[:tokens, :] = write[...]
        out[tokens : 2 * tokens, :] = read[...]
        for g in range(groups):
            at = 2 * tokens + g * heads
            out[at : at + heads, :] = logit[:, g * GROUP : (g + 1) * GROUP]
        lane = lax.broadcasted_iota(jnp.int32, (META_ROWS, LANES), 1)
        meta = jnp.zeros((META_ROWS, LANES), jnp.int32)
        for i in range(per):
            meta = jnp.where(lane == i, starts[i], meta)
            meta = jnp.where(lane == per + i, order[i] // GROUP, meta)
            meta = jnp.where(lane == 2 * per + i, order[i] % GROUP, meta)
        out[meta_at : meta_at + META_ROWS, :] = meta.astype(f32).astype(bf16)

    return run(
        body,
        (my,),
        (1,),
        [write_vector, read_vector, logits, doc_starts, block_order],
        [whole((tokens, state)), whole((tokens, state)), whole((heads, tokens))]
        + [pl.BlockSpec(memory_space=pltpu.SMEM)] * 2,
        jax.ShapeDtypeStruct((rows, LANES), bf16),
        whole((rows, LANES)),
        mib=4,
    )


def prep(my, extras, bias, rate_log, heads, tokens):
    members = len(extras)
    rows = extras[0].shape[0]
    total = members * tokens
    groups = tokens // GROUP
    all_heads = bias.shape[1]
    meta_at = 2 * tokens + groups * all_heads

    def body(my_ref, *refs):
        ex, (bias_ref, rate_ref) = refs[:members], refs[members : members + 2]
        write, read, dt_t, cum_t, cum_c, tail_c, table, ex_s, dt_s, cum_s = refs[members + 2 :]
        src = pl.program_id(0)

        def take(ref):
            ex_s[...] = ref[...]

        pick(src ^ my_ref[MEMBER], ex, take)
        write[...] = ex_s[:tokens, :]
        read[...] = ex_s[tokens : 2 * tokens, :]
        table[pl.ds(src, 1), :] = ex_s[meta_at : meta_at + 1, :].astype(
            f32
        ).astype(jnp.int32)
        upper = (
            lax.broadcasted_iota(jnp.int32, (GROUP, GROUP), 0)
            <= lax.broadcasted_iota(jnp.int32, (GROUP, GROUP), 1)
        ).astype(f32)
        bias_col = jnp.broadcast_to(bias_ref[...], (GROUP, all_heads)).T
        rate = jnp.exp(jnp.broadcast_to(rate_ref[...], (GROUP, all_heads)).T)
        mine = pl.ds(my_ref[MEMBER] * heads, heads)
        for g in range(groups):
            part = slice(g * GROUP, (g + 1) * GROUP)
            at = 2 * tokens + g * all_heads
            value = ex_s[at : at + all_heads, :].astype(f32) + bias_col
            step = jnp.maximum(value, 0.0) + jnp.log1p(jnp.exp(-jnp.abs(value)))
            dt_s[...] = step
            cum_s[...] = dot(-step * rate, upper, precision=highest)
            step = dt_s[mine, :]
            cumulative = cum_s[mine, :]
            dt_t[:, part] = step
            cum_t[:, part] = cumulative
            cum_c[part, :] = cumulative.T
            tail_c[part, :] = (jnp.exp(cumulative[:, GROUP - 1 :] - cumulative) * step).T

    return run(
        body,
        (my,),
        (members,),
        [*extras, bias, rate_log],
        [whole((rows, LANES))] * members + [whole((1, all_heads))] * 2,
        [
            jax.ShapeDtypeStruct((total, LANES), bf16),
            jax.ShapeDtypeStruct((total, LANES), bf16),
            jax.ShapeDtypeStruct((heads, total), f32),
            jax.ShapeDtypeStruct((heads, total), f32),
            jax.ShapeDtypeStruct((total, heads), f32),
            jax.ShapeDtypeStruct((total, heads), f32),
            jax.ShapeDtypeStruct((members, LANES), jnp.int32),
        ],
        [
            pl.BlockSpec((tokens, LANES), lambda i, my: (i, 0)),
            pl.BlockSpec((tokens, LANES), lambda i, my: (i, 0)),
            pl.BlockSpec((heads, tokens), lambda i, my: (0, i)),
            pl.BlockSpec((heads, tokens), lambda i, my: (0, i)),
            pl.BlockSpec((tokens, heads), lambda i, my: (i, 0)),
            pl.BlockSpec((tokens, heads), lambda i, my: (i, 0)),
            whole((members, LANES)),
        ],
        [
            pltpu.VMEM((rows, LANES), bf16),
            pltpu.VMEM((all_heads, GROUP), f32),
            pltpu.VMEM((all_heads, GROUP), f32),
        ],
        mib=10,
    )


def ssd(my, prepped, xs, gates, first, gain, offset, want_out):
    write, read, dt_t, cum_t, cum_c, tail_c, table = prepped
    members = len(xs)
    heads, total = dt_t.shape
    tokens, width = total // members, xs[0].shape[1]
    state = write.shape[1]
    groups = tokens // GROUP
    pairs = width // LANES
    head_of = LANES // HEAD_DIM
    table_rows = -(-members // META_ROWS) * META_ROWS
    base = offset // HEAD_DIM

    def body(my_ref, tab, *refs):
        refs = list(refs)
        x_refs = [refs.pop(0) for _ in range(members)]
        if want_out:
            g_refs = [refs.pop(0) for _ in range(members)]
            first_ref, gain_ref, read_ref, dtt, cumt = [refs.pop(0) for _ in range(5)]
        write_ref, cumc, tailc = [refs.pop(0) for _ in range(3)]
        table_ref = None if want_out else refs.pop(0)
        out = refs.pop(0)
        carry, x_s, scaled_s = [refs.pop(0) for _ in range(3)]
        g_s = refs.pop(0) if want_out else None
        src = pl.program_id(0)
        who = src ^ my_ref[MEMBER]

        @pl.when(src == 0)
        def _():
            if want_out:
                carry[...] = first_ref[...].astype(f32) * my_ref[SEGMENT].astype(f32)
            else:
                carry[...] = jnp.zeros_like(carry)

        def take_x(ref):
            x_s[...] = ref[...]

        pick(who, x_refs, take_x)
        if want_out:

            def take_g(ref):
                g_s[...] = ref[...]

            pick(who, g_refs, take_g)
            lower = lax.broadcasted_iota(jnp.int32, (GROUP, GROUP), 0) >= (
                lax.broadcasted_iota(jnp.int32, (GROUP, GROUP), 1)
            )
        left = lax.broadcasted_iota(jnp.int32, (GROUP, LANES), 1) < HEAD_DIM

        for g in range(groups):
            rows = slice(g * GROUP, (g + 1) * GROUP)
            writes = write_ref[rows, :]
            keep = 1.0 - tab[src, g].astype(f32)
            if want_out:
                reads = read_ref[rows, :]
                scores = dot(reads, writes, 1, 1)
                carried = dot(reads, (carry[...] * keep).astype(bf16))
            for p in range(pairs):
                lanes = slice(p * LANES, (p + 1) * LANES)
                h = base + head_of * p
                x = x_s[rows, lanes]
                xf = x.astype(f32)
                tail = jnp.where(left, tailc[rows, h : h + 1], tailc[rows, h + 1 : h + 2])
                scaled_s[:, lanes] = (xf * tail).astype(bf16)
                end = jnp.exp(
                    jnp.where(
                        left[:1],
                        cumc[rows.stop - 1 : rows.stop, h : h + 1],
                        cumc[rows.stop - 1 : rows.stop, h + 1 : h + 2],
                    )
                )
                if want_out:
                    cols = [cumc[rows, h + k : h + k + 1] for k in range(head_of)]
                    cum = jnp.where(left, cols[0], cols[1])
                    weights = []
                    for k in range(head_of):
                        gap = cols[k] - cumt[h + k : h + k + 1, rows]
                        decay = jnp.exp(jnp.where(lower, gap, -jnp.inf))
                        weights.append(
                            (scores * decay * dtt[h + k : h + k + 1, rows]).astype(bf16)
                        )
                    zero = jnp.zeros_like(x)
                    local = dot(
                        jnp.concatenate(weights, 1),
                        jnp.concatenate(
                            [jnp.where(left, x, zero), jnp.where(left, zero, x)], 0
                        ),
                    )
                    at = my_ref[MEMBER] * heads + h
                    skip = jnp.where(left[:1], gain_ref[at], gain_ref[at + 1])
                    mixed = local + jnp.exp(cum) * carried[:, lanes] + skip * xf
                    gate = g_s[rows, lanes].astype(f32)
                    out[rows, lanes] = (mixed * (gate / (1.0 + jnp.exp(-gate)))).astype(bf16)
                carry[:, lanes] = carry[:, lanes] * (end * keep)
            carry[...] += dot(writes, scaled_s[...], 0, 0)

        if not want_out:
            out[:state, :] = carry[...].astype(bf16)
            out[state:, :] = jnp.zeros((table_rows, width), bf16)
            out[state : state + members, :LANES] = table_ref[...].astype(f32).astype(bf16)

    by_rows = pl.BlockSpec((tokens, LANES), lambda i, *a: (i, 0))
    by_cols = pl.BlockSpec((heads, tokens), lambda i, *a: (0, i))
    by_head = pl.BlockSpec((tokens, heads), lambda i, *a: (i, 0))
    piece = whole((tokens, width))
    ins, in_specs = list(xs), [piece] * members
    below = pl.BlockSpec((tokens, width), lambda i, *a: (1, 0))
    if want_out:
        ins += [*gates, first, gain, read, dt_t, cum_t]
        in_specs += [below if gates is xs else piece] * members + [whole((state, width))]
        in_specs += [pl.BlockSpec(memory_space=pltpu.SMEM), by_rows, by_cols, by_cols]
    ins += [write, cum_c, tail_c]
    in_specs += [by_rows, by_head, by_head]
    scratch = [
        pltpu.VMEM((state, width), f32),
        pltpu.VMEM((tokens, width), bf16),
        pltpu.VMEM((GROUP, width), bf16),
    ]
    if want_out:
        outs = jax.ShapeDtypeStruct((members * tokens, width), bf16)
        out_specs = pl.BlockSpec((tokens, width), lambda i, *a: (i, 0))
        scratch.append(pltpu.VMEM((tokens, width), bf16))
    else:
        ins.append(table)
        in_specs.append(whole((members, LANES)))
        outs = jax.ShapeDtypeStruct((state + table_rows, width), bf16)
        out_specs = whole((state + table_rows, width))
    return run(
        body, (my, table), (members,), ins, in_specs, outs, out_specs, scratch,
        mib=14,
    )


def block_of(tables, my_ref, device, members, per, i):
    member = device % members
    same = device // members == my_ref[SEGMENT]
    high = jnp.where(same, tables[0][member, per + i], tables[1][member, per + i])
    low = jnp.where(same, tables[0][member, 2 * per + i], tables[1][member, 2 * per + i])
    return high * GROUP + low


def to_rows(my, tables, out, row_count, side, per):
    total, width = out.shape
    blocks = total // GROUP
    members = row_count * side // 2
    slots = side * per

    def body(my_ref, own, other, src, *refs):
        outs, sem = refs[:-1], refs[-1]

        def each(act):
            for s in range(row_count):
                row = my_ref[ROW] ^ s
                for q in range(slots):
                    block = block_of((own, other), my_ref, row * side + q // per, members, per, q % per)
                    start = pl.multiple_of((block % blocks) * GROUP, GROUP)
                    copy = pltpu.make_async_copy(
                        src.at[pl.ds(start, GROUP), :],
                        outs[s].at[pl.ds(q * GROUP, GROUP), :],
                        sem.at[s * slots + q],
                    )

                    @pl.when(block // blocks == my_ref[SEGMENT])
                    def _(copy=copy):
                        act(copy)

        each(lambda copy: copy.start())
        each(lambda copy: copy.wait())

    return run(
        body,
        (my, *tables),
        (1,),
        [out],
        [pl.BlockSpec(memory_space=pl.ANY)],
        [jax.ShapeDtypeStruct((slots * GROUP, width), bf16)] * row_count,
        [pl.BlockSpec(memory_space=pl.ANY)] * row_count,
        [pltpu.SemaphoreType.DMA((row_count * slots,))],
        mib=2,
    )


def to_cols(my, tables, received, side, per, c):
    row_count = len(received)
    width = received[0].shape[1]
    inner = row_count // 2
    members = inner * side
    blocks = members * per

    def body(my_ref, own, other, *refs):
        ins, out, sem = refs[:row_count], refs[row_count], refs[-1]
        col = my_ref[COL] ^ c
        for i in range(per):
            device = my_ref[ROW] * side + col
            segment = block_of((own, other), my_ref, device, members, per, i) // blocks
            start = pl.multiple_of((col * per + i) * GROUP, GROUP)
            for z in range(inner):

                def take(ref, i=i, z=z, start=start):
                    pltpu.make_async_copy(
                        ref.at[pl.ds(start, GROUP), :],
                        out.at[z, pl.ds(i * GROUP, GROUP), :],
                        sem.at[i * inner + z],
                    ).start()

                pick((segment * inner + z) ^ my_ref[ROW], ins, take)
        for i in range(per):
            for z in range(inner):
                pltpu.make_async_copy(
                    ins[0].at[pl.ds(0, GROUP), :],
                    out.at[z, pl.ds(i * GROUP, GROUP), :],
                    sem.at[i * inner + z],
                ).wait()

    return run(
        body,
        (my, *tables),
        (1,),
        received,
        [pl.BlockSpec(memory_space=pl.ANY)] * row_count,
        jax.ShapeDtypeStruct((inner, per * GROUP, width), bf16),
        pl.BlockSpec(memory_space=pl.ANY),
        [pltpu.SemaphoreType.DMA((per * inner,))],
        mib=2,
    )


def finish(my, pieces, norm_weight, tokens, features):
    side = len(pieces[0])
    inner = pieces[0][0].shape[0]
    widths = [row[0].shape[2] for row in pieces]
    columns = sum(widths)
    tile = GROUP
    flat = [piece for row in pieces for piece in row]

    def body(my_ref, *refs):
        ins, weight, out = refs[:-2], refs[-2], refs[-1]
        total = jnp.zeros((tile, LANES), f32)
        for ref in ins:
            for z in range(inner):
                value = ref[z].astype(f32)
                square = value * value
                for at in range(ref.shape[2] // LANES):
                    total = total + square[:, at * LANES : (at + 1) * LANES]
        scale = lax.rsqrt(jnp.sum(total, 1, keepdims=True) / features + 1e-05)
        for part, width in enumerate(widths):
            for c in range(side):
                for z in range(inner):
                    member = z * side + (my_ref[COL] ^ c)
                    start = pl.multiple_of(member * columns + sum(widths[:part]), LANES)
                    value = ins[part * side + c][z].astype(f32)
                    out[:, pl.ds(start, width)] = (
                        value * scale * weight[:, pl.ds(start, width)]
                    ).astype(bf16)

    return run(
        body,
        (my,),
        (tokens // tile,),
        [*flat, norm_weight[None, :]],
        [pl.BlockSpec((inner, tile, p.shape[2]), lambda i, *a: (0, i, 0)) for p in flat]
        + [whole((1, features))],
        jax.ShapeDtypeStruct((tokens, features), bf16),
        pl.BlockSpec((tile, features), lambda i, *a: (i, 0)),
        mib=8,
    )


def local(
    head_input,
    gate_input,
    write_vector,
    read_vector,
    increment_preactivation,
    step_bias,
    decay_log,
    skip_gain,
    norm_weight,
    doc_starts,
    block_order,
):
    devices = lax.axis_size("ctx")
    members = devices // 2
    row_count = devices // SIDE
    tokens, features = head_input.shape
    state = write_vector.shape[1]
    heads = step_bias.shape[0] // members
    columns = features // members
    plan = chunks(columns)
    per = doc_starts.shape[0]
    index = lax.axis_index("ctx")
    my = jnp.stack([index % members, index // members, index // SIDE, index % SIDE])
    my = my.astype(jnp.int32)

    def send(values, stride=1):
        moved = list(values)
        for s in range(1, len(values)):
            pairs = [(i, i ^ (s * stride)) for i in range(devices)]
            moved[s] = lax.ppermute(values[s], "ctx", pairs)
        return moved

    def in_hbm(value):
        return pltpu.with_memory_space_constraint(value, pltpu.HBM)

    x, gate = in_hbm(head_input), in_hbm(gate_input)
    small = gather_small(
        my,
        in_hbm(write_vector),
        in_hbm(read_vector),
        in_hbm(increment_preactivation.T),
        in_hbm(doc_starts),
        in_hbm(block_order),
    )
    extras = send([small] * members)
    sent = pack(my, [x], [((0,), *plan[0])], members, columns)
    x_parts = [send(sent[0])]
    wanted = [((1,), *plan[0])] + [((0, 1), *chunk) for chunk in plan[1:]]
    sent = pack(my, [x, gate], wanted, members, columns)
    g_parts = [send(sent[0])]
    for k in range(1, len(plan)):
        x_parts.append(send(sent[k]))
        g_parts.append(x_parts[k])
    prepped = prep(my, extras, step_bias[None, :], decay_log[None, :], heads, tokens)

    ends, firsts = [], []
    for k, (offset, width) in enumerate(plan):
        ends.append(ssd(my, prepped, x_parts[k], None, None, None, offset, False))
        swap = [(i, i ^ members) for i in range(devices)]
        firsts.append(lax.ppermute(ends[k], "ctx", swap))
    other = firsts[0][state : state + members, :LANES].astype(f32).astype(jnp.int32)
    tables = [prepped[-1], other]

    pieces = []
    for k, (offset, width) in enumerate(plan):
        out = ssd(my, prepped, x_parts[k], g_parts[k], firsts[k], skip_gain, offset, True)
        sent = to_rows(my, tables, out, row_count, SIDE, per)
        rows = send(sent, SIDE)
        sent = [to_cols(my, tables, rows, SIDE, per, c) for c in range(1, SIDE)]
        kept = to_cols(my, tables, rows, SIDE, per, 0)
        pieces.append(send([kept, *sent]))
    return finish(my, pieces, norm_weight, tokens, features)


def solution(mesh):
    rows = P(("dp", "ctx"), None)

    def whole_program(*args):
        step = jax.shard_map(
            local,
            mesh=mesh,
            in_specs=(rows,) * 5 + (P(),) * 4 + (P(("dp", "ctx")),) * 2,
            out_specs=rows,
            check_vma=False,
        )
        return step(*args)

    return whole_program
```

```python
import jax
import jax.numpy as jnp
from jax import lax
from jax.experimental import pallas as pl
from jax.experimental.pallas import tpu as pltpu
from jax.sharding import PartitionSpec as P


HEAD_DIM = 64
GROUP = 128
LANES = 128
META_ROWS = 16
CHUNKS = (256, 256, 256, 256)
SIDE = 2
UNROLL = 4
MEMBER, SEGMENT, ROW, COL = range(4)
MIB = 1024 * 1024

f32 = jnp.float32
bf16 = jnp.bfloat16
highest = lax.Precision.HIGHEST


def chunks(columns):
    if sum(CHUNKS) != columns:
        width = next(w for w in (256, 128) if columns % w == 0)
        return [(at, width) for at in range(0, columns, width)]
    return [(sum(CHUNKS[:k]), width) for k, width in enumerate(CHUNKS)]


def dot(left, right, left_dim=1, right_dim=0, precision=None):
    return lax.dot_general(
        left,
        right,
        (((left_dim,), (right_dim,)), ((), ())),
        precision=precision,
        preferred_element_type=f32,
    )


def run(body, scalars, grid, ins, in_specs, outs, out_specs, scratch=(), mib=8):
    return pl.pallas_call(
        body,
        grid_spec=pltpu.PrefetchScalarGridSpec(
            num_scalar_prefetch=len(scalars),
            grid=grid,
            in_specs=in_specs,
            out_specs=out_specs,
            scratch_shapes=list(scratch),
        ),
        out_shape=outs,
        compiler_params=pltpu.CompilerParams(
            dimension_semantics=("arbitrary",) * len(grid),
            vmem_limit_bytes=mib * MIB,
        ),
    )(*scalars, *ins)


def whole(shape):
    return pl.BlockSpec(shape, lambda *a: (0,) * len(shape))


def pick(step, refs, take):
    for number, ref in enumerate(refs):

        @pl.when(step == number)
        def _(ref=ref):
            take(ref)


def pack(my, arrays, wanted, members, columns, after=()):
    tokens = arrays[0].shape[0]
    total = members * sum(len(numbers) for numbers, _, _ in wanted)

    def body(my_ref, *refs):
        outs, sem = refs[-members * len(wanted) - 1 : -1], refs[-1]
        copies = []
        for w, (numbers, offset, width) in enumerate(wanted):
            for s in range(members):
                start = pl.multiple_of((my_ref[MEMBER] ^ s) * columns + offset, LANES)
                for a, number in enumerate(numbers):
                    copies.append(
                        pltpu.make_async_copy(
                            refs[number].at[:, pl.ds(start, width)],
                            outs[w * members + s].at[pl.ds(a * tokens, tokens), :],
                            sem.at[len(copies)],
                        )
                    )
        for copy in copies:
            copy.start()
        for copy in copies:
            copy.wait()

    out = run(
        body,
        (my,),
        (1,),
        [*arrays, *after],
        [pl.BlockSpec(memory_space=pl.ANY)] * (len(arrays) + len(after)),
        [
            jax.ShapeDtypeStruct((len(numbers) * tokens, width), arrays[0].dtype)
            for numbers, _, width in wanted
            for _ in range(members)
        ],
        [pl.BlockSpec(memory_space=pl.ANY)] * (members * len(wanted)),
        [pltpu.SemaphoreType.DMA((total,))],
        mib=2,
    )
    return [out[w * members : (w + 1) * members] for w in range(len(wanted))]


def gather_small(my, write_vector, read_vector, logits, doc_starts, block_order):
    tokens, state = write_vector.shape
    heads = logits.shape[0]
    groups = tokens // GROUP
    per = doc_starts.shape[0]
    meta_at = 2 * tokens + groups * heads
    rows = meta_at + META_ROWS

    def body(my_ref, write, read, logit, starts, order, out):
        out[:tokens, :] = write[...]
        out[tokens : 2 * tokens, :] = read[...]
        for g in range(groups):
            at = 2 * tokens + g * heads
            out[at : at + heads, :] = logit[:, g * GROUP : (g + 1) * GROUP]
        lane = lax.broadcasted_iota(jnp.int32, (META_ROWS, LANES), 1)
        meta = jnp.zeros((META_ROWS, LANES), jnp.int32)
        for i in range(per):
            meta = jnp.where(lane == i, starts[i], meta)
            meta = jnp.where(lane == per + i, order[i] // GROUP, meta)
            meta = jnp.where(lane == 2 * per + i, order[i] % GROUP, meta)
        out[meta_at : meta_at + META_ROWS, :] = meta.astype(f32).astype(bf16)

    return run(
        body,
        (my,),
        (1,),
        [write_vector, read_vector, logits, doc_starts, block_order],
        [whole((tokens, state)), whole((tokens, state)), whole((heads, tokens))]
        + [pl.BlockSpec(memory_space=pltpu.SMEM)] * 2,
        jax.ShapeDtypeStruct((rows, LANES), bf16),
        whole((rows, LANES)),
        mib=4,
    )


def prep(my, extras, bias, rate_log, heads, tokens):
    members = len(extras)
    rows = extras[0].shape[0]
    total = members * tokens
    groups = tokens // GROUP
    all_heads = bias.shape[1]
    meta_at = 2 * tokens + groups * all_heads

    def body(my_ref, *refs):
        ex, (bias_ref, rate_ref) = refs[:members], refs[members : members + 2]
        write, read, dt_t, cum_t, cum_c, tail_c, table, ex_s, dt_s, cum_s = refs[members + 2 :]
        src = pl.program_id(0)

        def take(ref):
            ex_s[...] = ref[...]

        pick(src ^ my_ref[MEMBER], ex, take)
        write[...] = ex_s[:tokens, :]
        read[...] = ex_s[tokens : 2 * tokens, :]
        table[pl.ds(src, 1), :] = ex_s[meta_at : meta_at + 1, :].astype(
            f32
        ).astype(jnp.int32)
        upper = (
            lax.broadcasted_iota(jnp.int32, (GROUP, GROUP), 0)
            <= lax.broadcasted_iota(jnp.int32, (GROUP, GROUP), 1)
        ).astype(f32)
        bias_col = jnp.broadcast_to(bias_ref[...], (GROUP, all_heads)).T
        rate = jnp.exp(jnp.broadcast_to(rate_ref[...], (GROUP, all_heads)).T)
        mine = pl.ds(my_ref[MEMBER] * heads, heads)
        for g in range(groups):
            part = slice(g * GROUP, (g + 1) * GROUP)
            at = 2 * tokens + g * all_heads
            value = ex_s[at : at + all_heads, :].astype(f32) + bias_col
            step = jnp.maximum(value, 0.0) + jnp.log1p(jnp.exp(-jnp.abs(value)))
            dt_s[...] = step
            cum_s[...] = dot(-step * rate, upper, precision=highest)
            step = dt_s[mine, :]
            cumulative = cum_s[mine, :]
            dt_t[:, part] = step
            cum_t[:, part] = cumulative
            cum_c[part, :] = cumulative.T
            tail_c[part, :] = (jnp.exp(cumulative[:, GROUP - 1 :] - cumulative) * step).T

    return run(
        body,
        (my,),
        (members,),
        [*extras, bias, rate_log],
        [whole((rows, LANES))] * members + [whole((1, all_heads))] * 2,
        [
            jax.ShapeDtypeStruct((total, LANES), bf16),
            jax.ShapeDtypeStruct((total, LANES), bf16),
            jax.ShapeDtypeStruct((heads, total), f32),
            jax.ShapeDtypeStruct((heads, total), f32),
            jax.ShapeDtypeStruct((total, heads), f32),
            jax.ShapeDtypeStruct((total, heads), f32),
            jax.ShapeDtypeStruct((members, LANES), jnp.int32),
        ],
        [
            pl.BlockSpec((tokens, LANES), lambda i, my: (i, 0)),
            pl.BlockSpec((tokens, LANES), lambda i, my: (i, 0)),
            pl.BlockSpec((heads, tokens), lambda i, my: (0, i)),
            pl.BlockSpec((heads, tokens), lambda i, my: (0, i)),
            pl.BlockSpec((tokens, heads), lambda i, my: (i, 0)),
            pl.BlockSpec((tokens, heads), lambda i, my: (i, 0)),
            whole((members, LANES)),
        ],
        [
            pltpu.VMEM((rows, LANES), bf16),
            pltpu.VMEM((all_heads, GROUP), f32),
            pltpu.VMEM((all_heads, GROUP), f32),
        ],
        mib=10,
    )


def block_of(tables, my_ref, device, members, per, i):
    member = device % members
    same = device // members == my_ref[SEGMENT]
    high = jnp.where(same, tables[0][member, per + i], tables[1][member, per + i])
    low = jnp.where(same, tables[0][member, 2 * per + i], tables[1][member, 2 * per + i])
    return high * GROUP + low


def ssd(my, tables, prepped, xs, gates, first, gain, offset, row_count, side, per):
    write, read, dt_t, cum_t, cum_c, tail_c = prepped
    members = len(xs)
    heads, total = dt_t.shape
    tokens, width = total // members, xs[0].shape[1]
    state = write.shape[1]
    groups = tokens // GROUP
    blocks = total // GROUP
    slots = side * per
    pairs = width // LANES
    head_of = LANES // HEAD_DIM
    table_rows = -(-members // META_ROWS) * META_ROWS
    base = offset // HEAD_DIM
    want_out = gates is not None

    def body(*refs):
        refs = list(refs)
        my_ref = refs.pop(0)
        tabs = [refs.pop(0) for _ in tables]
        x_refs = [refs.pop(0) for _ in range(members)]
        if want_out:
            g_refs = [refs.pop(0) for _ in range(members)]
            first_ref, gain_ref, read_ref, dtt, cumt = [refs.pop(0) for _ in range(5)]
        write_ref, cumc, tailc = [refs.pop(0) for _ in range(3)]
        if want_out:
            outs = [refs.pop(0) for _ in range(row_count)]
            carry, x_s, scaled_s, g_s, out_s, sem = refs
            carry[...] = first_ref[...].astype(f32) * my_ref[SEGMENT].astype(f32)
        else:
            table_ref, out, carry, x_s, scaled_s = refs
            carry[...] = jnp.zeros_like(carry)
        left = lax.broadcasted_iota(jnp.int32, (GROUP, LANES), 1) < HEAD_DIM
        lower = lax.broadcasted_iota(jnp.int32, (GROUP, GROUP), 0) >= (
            lax.broadcasted_iota(jnp.int32, (GROUP, GROUP), 1)
        )

        def in_order(src, unused):
            here = pl.ds(pl.multiple_of(src * tokens, GROUP), tokens)
            who = src ^ my_ref[MEMBER]

            def take_x(ref):
                x_s[here, :] = ref[...]

            pick(who, x_refs, take_x)
            if want_out:

                def take_g(ref):
                    g_s[here, :] = ref[...]

                pick(who, g_refs, take_g)
            return unused

        lax.fori_loop(0, members, in_order, 0)

        def each_source(src, unused):
            for g in range(groups):
                at = pl.multiple_of(src * tokens + g * GROUP, GROUP)
                there = pl.ds(at, GROUP)
                writes = write_ref[there, :]
                keep = 1.0 - tabs[0][src, g].astype(f32)
                cum_all = cumc[there, :]
                tail_all = tailc[there, :]
                if want_out:
                    reads = read_ref[there, :]
                    scores = dot(reads, writes, 1, 1)
                    carried = dot(reads, (carry[...] * keep).astype(bf16))
                    cum_rows = cumt[:, there]
                    step_rows = dtt[:, there]
                for p in range(pairs):
                    lanes = slice(p * LANES, (p + 1) * LANES)
                    h = base + head_of * p
                    x = x_s[there, lanes]
                    xf = x.astype(f32)
                    tail = jnp.where(left, tail_all[:, h : h + 1], tail_all[:, h + 1 : h + 2])
                    scaled_s[:, lanes] = (xf * tail).astype(bf16)
                    cols = [cum_all[:, h + k : h + k + 1] for k in range(head_of)]
                    end = jnp.exp(
                        jnp.where(left[:1], cols[0][GROUP - 1 :], cols[1][GROUP - 1 :])
                    )
                    if want_out:
                        cum = jnp.where(left, cols[0], cols[1])
                        weights = []
                        for k in range(head_of):
                            gap = cols[k] - cum_rows[h + k : h + k + 1, :]
                            decay = jnp.exp(jnp.where(lower, gap, -jnp.inf))
                            weights.append(
                                (scores * decay * step_rows[h + k : h + k + 1, :]).astype(bf16)
                            )
                        zero = jnp.zeros_like(x)
                        local = dot(
                            jnp.concatenate(weights, 1),
                            jnp.concatenate(
                                [jnp.where(left, x, zero), jnp.where(left, zero, x)], 0
                            ),
                        )
                        skip_at = my_ref[MEMBER] * heads + h
                        skip = jnp.where(left[:1], gain_ref[skip_at], gain_ref[skip_at + 1])
                        mixed = local + jnp.exp(cum) * carried[:, lanes] + skip * xf
                        gate = g_s[there, lanes].astype(f32)
                        out_s[there, lanes] = (mixed * (gate / (1.0 + jnp.exp(-gate)))).astype(bf16)
                    carry[:, lanes] = carry[:, lanes] * (end * keep)
                carry[...] += dot(writes, scaled_s[...], 0, 0)
            return unused

        lax.fori_loop(0, members, each_source, 0, unroll=members if members <= UNROLL else 1)
        if not want_out:
            out[:state, :] = carry[...].astype(bf16)
            out[state:, :] = jnp.zeros((table_rows, width), bf16)
            out[state : state + members, :LANES] = table_ref[...].astype(f32).astype(bf16)
            return

        def each_slot(act):
            for s in range(row_count):
                row = my_ref[ROW] ^ s
                for q in range(slots):
                    block = block_of(tabs, my_ref, row * side + q // per, members, per, q % per)
                    start = pl.multiple_of((block % blocks) * GROUP, GROUP)
                    copy = pltpu.make_async_copy(
                        out_s.at[pl.ds(start, GROUP), :],
                        outs[s].at[pl.ds(q * GROUP, GROUP), :],
                        sem.at[s * slots + q],
                    )

                    @pl.when(block // blocks == my_ref[SEGMENT])
                    def _(copy=copy):
                        act(copy)

        each_slot(lambda copy: copy.start())
        each_slot(lambda copy: copy.wait())

    piece = whole((tokens, width))
    ins, in_specs = list(xs), [piece] * members
    below = pl.BlockSpec((tokens, width), lambda i, *a: (1, 0))
    if want_out:
        ins += [*gates, first, gain, read, dt_t, cum_t]
        in_specs += [below if gates is xs else piece] * members + [whole((state, width))]
        in_specs += [pl.BlockSpec(memory_space=pltpu.SMEM)]
        in_specs += [whole((total, LANES))] + [whole((heads, total))] * 2
    ins += [write, cum_c, tail_c]
    in_specs += [whole((total, LANES))] + [whole((total, heads))] * 2
    scratch = [
        pltpu.VMEM((state, width), f32),
        pltpu.VMEM((total, width), bf16),
        pltpu.VMEM((GROUP, width), bf16),
    ]
    if want_out:
        outs = [jax.ShapeDtypeStruct((slots * GROUP, width), bf16)] * row_count
        out_specs = [pl.BlockSpec(memory_space=pl.ANY)] * row_count
        scratch += [
            pltpu.VMEM((total, width), bf16),
            pltpu.VMEM((total, width), bf16),
            pltpu.SemaphoreType.DMA((row_count * slots,)),
        ]
    else:
        ins.append(tables[0])
        in_specs.append(whole((members, LANES)))
        outs = jax.ShapeDtypeStruct((state + table_rows, width), bf16)
        out_specs = whole((state + table_rows, width))
    return run(
        body, (my, *tables), (1,), ins, in_specs, outs, out_specs, scratch,
        mib=12 + 40 * blocks // 64,
    )


def to_cols(my, tables, received, side, per, c):
    row_count = len(received)
    width = received[0].shape[1]
    inner = row_count // 2
    members = inner * side
    blocks = members * per

    def body(my_ref, own, other, *refs):
        ins, out, sem = refs[:row_count], refs[row_count], refs[-1]
        col = my_ref[COL] ^ c
        for i in range(per):
            device = my_ref[ROW] * side + col
            segment = block_of((own, other), my_ref, device, members, per, i) // blocks
            start = pl.multiple_of((col * per + i) * GROUP, GROUP)
            for z in range(inner):

                def take(ref, i=i, z=z, start=start):
                    pltpu.make_async_copy(
                        ref.at[pl.ds(start, GROUP), :],
                        out.at[z, pl.ds(i * GROUP, GROUP), :],
                        sem.at[i * inner + z],
                    ).start()

                pick((segment * inner + z) ^ my_ref[ROW], ins, take)
        for i in range(per):
            for z in range(inner):
                pltpu.make_async_copy(
                    ins[0].at[pl.ds(0, GROUP), :],
                    out.at[z, pl.ds(i * GROUP, GROUP), :],
                    sem.at[i * inner + z],
                ).wait()

    return run(
        body,
        (my, *tables),
        (1,),
        received,
        [pl.BlockSpec(memory_space=pl.ANY)] * row_count,
        jax.ShapeDtypeStruct((inner, per * GROUP, width), bf16),
        pl.BlockSpec(memory_space=pl.ANY),
        [pltpu.SemaphoreType.DMA((per * inner,))],
        mib=2,
    )


def finish(my, pieces, norm_weight, tokens, features):
    side = len(pieces[0])
    inner = pieces[0][0].shape[0]
    widths = [row[0].shape[2] for row in pieces]
    columns = sum(widths)
    tile = GROUP
    flat = [piece for row in pieces for piece in row]

    def body(my_ref, *refs):
        ins, weight, out = refs[:-2], refs[-2], refs[-1]
        total = jnp.zeros((tile, LANES), f32)
        for ref in ins:
            for z in range(inner):
                value = ref[z].astype(f32)
                square = value * value
                for at in range(ref.shape[2] // LANES):
                    total = total + square[:, at * LANES : (at + 1) * LANES]
        scale = lax.rsqrt(jnp.sum(total, 1, keepdims=True) / features + 1e-05)
        for part, width in enumerate(widths):
            for c in range(side):
                for z in range(inner):
                    member = z * side + (my_ref[COL] ^ c)
                    start = pl.multiple_of(member * columns + sum(widths[:part]), LANES)
                    value = ins[part * side + c][z].astype(f32)
                    out[:, pl.ds(start, width)] = (
                        value * scale * weight[:, pl.ds(start, width)]
                    ).astype(bf16)

    return run(
        body,
        (my,),
        (tokens // tile,),
        [*flat, norm_weight[None, :]],
        [pl.BlockSpec((inner, tile, p.shape[2]), lambda i, *a: (0, i, 0)) for p in flat]
        + [whole((1, features))],
        jax.ShapeDtypeStruct((tokens, features), bf16),
        pl.BlockSpec((tile, features), lambda i, *a: (i, 0)),
        mib=8,
    )


def local(
    head_input,
    gate_input,
    write_vector,
    read_vector,
    increment_preactivation,
    step_bias,
    decay_log,
    skip_gain,
    norm_weight,
    doc_starts,
    block_order,
):
    devices = lax.axis_size("ctx")
    members = devices // 2
    row_count = devices // SIDE
    tokens, features = head_input.shape
    state = write_vector.shape[1]
    heads = step_bias.shape[0] // members
    columns = features // members
    plan = chunks(columns)
    per = doc_starts.shape[0]
    index = lax.axis_index("ctx")
    my = jnp.stack([index % members, index // members, index // SIDE, index % SIDE])
    my = my.astype(jnp.int32)

    def send(values, stride=1):
        moved = list(values)
        for s in range(1, len(values)):
            pairs = [(i, i ^ (s * stride)) for i in range(devices)]
            moved[s] = lax.ppermute(values[s], "ctx", pairs)
        return moved

    def in_hbm(value):
        return pltpu.with_memory_space_constraint(value, pltpu.HBM)

    x, gate = in_hbm(head_input), in_hbm(gate_input)
    small = gather_small(
        my,
        in_hbm(write_vector),
        in_hbm(read_vector),
        in_hbm(increment_preactivation.T),
        in_hbm(doc_starts),
        in_hbm(block_order),
    )
    extras = send([small] * members)
    sent = pack(my, [x], [((0,), *plan[0])], members, columns)
    x_parts = [send(sent[0])]
    wanted = [((1,), *plan[0])] + [((0, 1), *chunk) for chunk in plan[1:]]
    sent = pack(my, [x, gate], wanted, members, columns)
    g_parts = [send(sent[0])]
    for k in range(1, len(plan)):
        x_parts.append(send(sent[k]))
        g_parts.append(x_parts[k])
    *prepped, table = prep(my, extras, step_bias[None, :], decay_log[None, :], heads, tokens)
    places = (row_count, SIDE, per)

    ends, firsts = [], []
    for k, (offset, width) in enumerate(plan):
        ends.append(ssd(my, [table], prepped, x_parts[k], None, None, None, offset, *places))
        swap = [(i, i ^ members) for i in range(devices)]
        firsts.append(lax.ppermute(ends[k], "ctx", swap))
    other = firsts[0][state : state + members, :LANES].astype(f32).astype(jnp.int32)
    tables = [table, other]

    pieces = []
    for k, (offset, width) in enumerate(plan):
        sent = ssd(
            my, tables, prepped, x_parts[k], g_parts[k], firsts[k], skip_gain, offset, *places
        )
        rows = send(sent, SIDE)
        sent = [to_cols(my, tables, rows, SIDE, per, c) for c in range(1, SIDE)]
        kept = to_cols(my, tables, rows, SIDE, per, 0)
        pieces.append(send([kept, *sent]))
    return finish(my, pieces, norm_weight, tokens, features)


def solution(mesh):
    rows = P(("dp", "ctx"), None)

    def whole_program(*args):
        step = jax.shard_map(
            local,
            mesh=mesh,
            in_specs=(rows,) * 5 + (P(),) * 4 + (P(("dp", "ctx")),) * 2,
            out_specs=rows,
            check_vma=False,
        )
        return step(*args)

    return whole_program
```
